32 devices in a mesh: grp: 4 (over x, core), row: 8 (over z, y).
Axes of the slice: x: 2, y: 2, z: 4, core: 2. Of those that a mesh axis runs over, the one named last changes fastest.
Arguments:
- placing: int32 [1024], P('grp'), parts along dimension 0, may hold values from 0 to 255, as said below
- lengths: int32 [64], P('grp'), parts along dimension 0, may hold values from 1 to 48, 256 in all
- diag_blocks: float32 [1024, 128, 128], P(('grp', 'row')), parts along dimension 0, as said below
- lower_blocks: float32 [1024, 128, 128], P(('grp', 'row')), parts along dimension 0, may hold values from -0.25 to 0.25
- right_side: float32 [1024, 128, 128], P(('grp', 'row')), parts along dimension 0, may hold values from -6 to 6
Outputs:
- solution: float32 [1024, 128, 128], P(('grp', 'row')), parts along dimension 0
- residual: float32 [1024, 128, 128], P(('grp', 'row')), parts along dimension 0
The draws below stay inside these ranges and needn't reach their ends.
There are 4 independent parts, one for each index of `grp`. The reference program is written for one: setup_inputs(seed, part) draws one part's arguments, and reference() takes and returns one part's arrays. A program takes and returns all parts, laid end to end along the dimension named above; each array names one. Nothing has to cross between parts.
Inputs may be any that keep to these rules, and one draw needn't show every extreme that they name: `placing`: A permutation of 0 .. 255. Device d holds the slots d * 32 .. (d + 1) * 32 - 1, and among them exactly 4 name block rows of each range e * 32 .. (e + 1) * 32 - 1. `lengths`: they sum to 256. `diag_blocks`: every block is symmetric, and the assembled operator of every system is positive definite.
All inputs are finite; a program needn't handle non-finite values.
Results may differ from the reference program's by a relative error of at most 0.0003.
Values sent between devices are 32-bit elements; how exact they have to be, the bound alone decides.
No kernel may reach another device: no remote copies, remote signals or barrier semaphores. Data moves between devices by JAX's collectives and lax.ppermute only.
A program may use at most 128 MiB of HBM per device.

```python
import math
import jax
import jax.numpy as jnp
import numpy as np
from jax import lax

B = 128
K = 128
BPD = 32
ITERS = 4
NB = 256
SYSTEMS = 16
MOSTLEN = 48


def shuffle_one(subkey):
    return jax.random.permutation(subkey, BPD)


def draw_placing(key, part):
    groups = NB // BPD
    share_rows = BPD // groups
    first_key, second_key = jax.random.split(jax.random.fold_in(key, 11))
    shuffled = jax.vmap(shuffle_one)(jax.random.split(first_key, groups)).astype(jnp.int32)
    owned = shuffled + (jnp.arange(groups, dtype=jnp.int32) * BPD)[:, None]
    spread_out = owned.reshape(groups, groups, share_rows).transpose(1, 0, 2).reshape(groups, BPD)
    mixing = jax.vmap(shuffle_one)(jax.random.split(second_key, groups)).astype(jnp.int32)
    return jnp.take_along_axis(spread_out, mixing, axis=1).reshape(NB).astype(jnp.int32)


def draw_diag_blocks(key, part):
    first_key, second_key = jax.random.split(jax.random.fold_in(key, 23))
    raw_part = jax.random.normal(first_key, (NB, B, B), jnp.float32) * (0.5 / B ** 0.5)
    shifts = jax.random.uniform(second_key, (NB,), jnp.float32, 5.0, 10.0)
    identity = jnp.eye(B, dtype=jnp.float32)
    blocks = raw_part + jnp.swapaxes(raw_part, 1, 2) + shifts[:, None, None] * identity[None, :, :]
    return blocks.astype(jnp.float32)


def block_scale(rng, extent, cuts, low, high):
    loudness = 1.0
    for dim, blocks in cuts:
        draws = jax.random.uniform(jax.random.fold_in(jax.random.fold_in(rng, 6), dim), (blocks,), jnp.float32, low / len(cuts), high / len(cuts))
        loudness = loudness * jnp.repeat(jnp.exp(draws), extent[dim] // blocks).reshape((-1,) + (1,) * (len(extent) - 1 - dim))
    return loudness


def length_profile(amount, total, most, lean):
    loads = [(1 << 20) // math.isqrt(rank ** lean) + 1 for rank in range(2, amount + 1)]
    surplus, holding = total - most - (amount - 1), [1] * (amount - 1)
    while surplus > 0:
        free = [i for i in range(amount - 1) if holding[i] < most]
        whole, left = sum([loads[i] for i in free]), surplus
        for i in free:
            extra = min(most - holding[i], max(1, left * loads[i] // whole), surplus)
            holding[i] = holding[i] + extra
            surplus = surplus - extra
    return np.array([most] + holding)


def uneven_parts(rng, number_of, total, reach, lean):
    if number_of == 2:
        one = jax.random.randint(rng, (), max(1, total - reach), min(reach, total - 1) + 1)
        return jnp.stack([one, total - one])
    tallies = jnp.asarray(length_profile(number_of, total, reach, lean), jnp.int32)
    pairs = (number_of - 1) // 2
    giver, taker = tallies[1:1 + 2 * pairs:2], tallies[2:2 + 2 * pairs:2]
    slack = jnp.minimum(giver - 1, reach - taker)
    shifted = jax.random.randint(jax.random.fold_in(rng, 1), (pairs,), 0, 1 << 20) % (slack + 1)
    tallies = tallies.at[1:1 + 2 * pairs:2].set(giver - shifted).at[2:2 + 2 * pairs:2].set(taker + shifted)
    return tallies[jax.random.permutation(jax.random.fold_in(rng, 2), number_of)]


def bell_draw(key, shape, deviation, most, cuts=(), held_as=jnp.bfloat16):
    array = jax.random.normal(key, shape, jnp.float32) * deviation
    if len(cuts) > 0:
        array = block_scale(key, shape, cuts, -0.22, 0.18) * array
    return jnp.clip(array, min=-most, max=most).astype(held_as)


def setup_inputs(seed: int = 0, part: int = 0) -> dict:
    streams_of = jax.random.split(jax.random.key(seed), 6)
    own_keys = jax.random.split(jax.random.fold_in(streams_of[5], part), 6)
    return {
        "placing": draw_placing(jax.random.fold_in(jax.random.fold_in(streams_of[5], part), 71), part),
        "lengths": uneven_parts(own_keys[1], SYSTEMS, NB, MOSTLEN, 2).astype(jnp.int32),
        "diag_blocks": draw_diag_blocks(jax.random.fold_in(jax.random.fold_in(streams_of[5], part), 71), part),
        "lower_blocks": bell_draw(own_keys[3], (NB, B, B), (4 * B) ** -0.5, 0.25, ((0, 8),), jnp.float32),
        "right_side": bell_draw(own_keys[4], (NB, B, K), 1.0, 6.0, ((0, 8),), jnp.float32),
    }


HIGHEST = lax.Precision.HIGHEST


def reference(placing, lengths, diag_blocks, lower_blocks, right_side):
    inverse = jnp.argsort(placing, stable=True).astype(jnp.int32)
    diagonal = diag_blocks[inverse]
    coupling_raw = lower_blocks[inverse]
    rhs_nat = right_side[inverse]
    seg_ends = jnp.cumsum(lengths).astype(jnp.int32)
    starts = seg_ends - lengths
    global_rows = jnp.arange(NB, dtype=jnp.int32)
    segment = jnp.sum((global_rows[:, None] >= seg_ends[None, :]).astype(jnp.int32), axis=1).astype(jnp.int32)
    is_first = jnp.any(global_rows[:, None] == starts[None, :], axis=1)
    keep_mask = jnp.where(is_first, 0.0, 1.0).astype(jnp.float32)
    coupling_low = coupling_raw * keep_mask[:, None, None]

    def operate(field):
        center = jnp.einsum('jab,jbk->jak', diagonal, field, precision=HIGHEST)
        shifted_down = jnp.concatenate([jnp.zeros_like(field[:1]), field[:-1]], axis=0)
        from_below = jnp.einsum('jab,jbk->jak', coupling_low, shifted_down, precision=HIGHEST)
        turned = jnp.einsum('jba,jbk->jak', coupling_low, field, precision=HIGHEST)
        from_above = jnp.concatenate([turned[1:], jnp.zeros_like(turned[:1])], axis=0)
        return center + from_below + from_above

    def per_system(values):
        return jax.ops.segment_sum(jnp.sum(values, axis=1), segment, num_segments=SYSTEMS)

    def spread(coefficient):
        return coefficient[segment][:, None, :]

    solution = jnp.zeros_like(rhs_nat)
    residual = rhs_nat
    direction = rhs_nat
    norm_now = per_system(residual * residual)
    for iteration in range(ITERS):
        image = operate(direction)
        step_size = norm_now / per_system(direction * image)
        solution = solution + spread(step_size) * direction
        residual = residual - spread(step_size) * image
        norm_next = per_system(residual * residual)
        direction = residual + spread(norm_next / norm_now) * direction
        norm_now = norm_next
    return solution, residual
```

```python
import functools

import jax
import jax.numpy as jnp
from jax import lax
from jax.experimental import pallas as pl
from jax.experimental.pallas import tpu as pltpu
from jax.sharding import PartitionSpec as P

ITERS = 4
MOSTLEN = 48


F32 = jnp.float32
BF16 = jnp.bfloat16
ANY = pl.BlockSpec(memory_space=pl.ANY)
VMEM = pl.BlockSpec(memory_space=pltpu.VMEM)
SMEM = pl.BlockSpec(memory_space=pltpu.SMEM)
HBM = pl.BlockSpec(memory_space=pltpu.HBM)
MIB = 1 << 20
GATE = 0
UNROLL = 10


def shifted(x, by):
    count = lax.axis_size("row")
    return lax.ppermute(x, "row", [(i, (i + by) % count) for i in range(count)])


def swapped(x, by, phase):
    count = lax.axis_size("row")
    pairs = [(i, i + by if (i // by + phase) % 2 == 0 else i - by) for i in range(count)]
    return lax.ppermute(x, "row", [(i, j) for i, j in pairs if 0 <= j < count])


def sds(shape, dtype=F32):
    return jax.ShapeDtypeStruct(shape, dtype)


def in_hbm(x):
    return pltpu.with_memory_space_constraint(x, pltpu.HBM)


def call(kernel, out_shape, in_specs, out_specs, scratch=(), vmem=20, flops=1000000, **extra):
    return pl.pallas_call(
        kernel,
        out_shape=out_shape,
        in_specs=in_specs,
        out_specs=out_specs,
        scratch_shapes=list(scratch),
        compiler_params=pltpu.CompilerParams(vmem_limit_bytes=vmem * MIB),
        cost_estimate=pl.CostEstimate(flops=flops, transcendentals=0, bytes_accessed=0),
        **extra,
    )


def split(x):
    high = x.astype(BF16)
    return high, (x - high.astype(F32)).astype(BF16)


def pack_coupled(count, share, placing, lower, rhs, *rest):
    outs, order, (seen, sems) = rest[:count], rest[count], rest[count + 1 :]
    device = lax.axis_index("row")
    per_dev = count * share
    for k in range(count):
        seen[k] = 0

    def rank(s, carry):
        target = lax.div(placing[device * per_dev + s], per_dev)
        k = lax.rem(target - device + count, count)
        order[k * share + seen[k]] = s
        seen[k] = seen[k] + 1
        return carry

    lax.fori_loop(0, per_dev, rank, 0, unroll=8)
    copies = []
    for q in range(per_dev):
        k, r = divmod(q, share)
        copies.append(pltpu.make_async_copy(lower.at[order[q]], outs[k].at[r], sems.at[2 * q]))
        copies.append(pltpu.make_async_copy(rhs.at[order[q]], outs[k].at[share + r], sems.at[2 * q + 1]))
    for copy in copies:
        copy.start()
    for copy in copies:
        copy.wait()


def pack_diag(count, share, order, diag, gate, *rest):
    outs, held, sems = rest[:count], rest[count], rest[count + 1]
    size = diag.shape[1]
    half = size // 2
    per_dev = count * share

    def fetch(q):
        return pltpu.make_async_copy(diag.at[order[q]], held.at[q], sems.at[q])

    for q in range(per_dev):
        fetch(q).start()
    across = lax.broadcasted_iota(jnp.int32, (half, size), 1)
    down = lax.broadcasted_iota(jnp.int32, (half, size), 0)
    eye = lax.broadcasted_iota(jnp.int32, (size, size), 0) == lax.broadcasted_iota(jnp.int32, (size, size), 1)
    lane = lax.broadcasted_iota(jnp.int32, (1, size), 1)
    traces = jnp.zeros((1, size), F32)
    for k in range(count):
        for r in range(share):
            q = k * share + r
            fetch(q).wait()
            block = held[q]
            top, turned = block[:half], pltpu.roll(block[half:], half, 1)
            outs[k][r * half : (r + 1) * half, :] = jnp.where(
                across >= half, top, jnp.where(across > down, top, turned)
            )
            along = jnp.sum(jnp.where(eye, block, 0.0), axis=0, keepdims=True)
            outs[k][share * half + r : share * half + r + 1, :] = along
            traces = jnp.where(lane == order[q], jnp.sum(along, axis=1, keepdims=True), traces)
    for k in range(count):
        outs[k][share * half + share : share * half + share + 1, :] = traces


def unpack_coupled(count, share, dest, keep, *rest):
    arrived = rest[:count]
    rhs, low, low_t, to_left, to_right, chunks, sems = rest[count:]
    per_dev = rhs.shape[0]
    copies = [pltpu.make_async_copy(arrived[k], chunks.at[k], sems.at[k]) for k in range(count)]
    for copy in copies:
        copy.start()
    for k in range(count):

        def place(r, carry, k=k):
            row = dest[k * share + r]
            block = jnp.where(keep[row] > 0, chunks[k, r], 0.0)
            low[row] = jnp.concatenate(split(block), axis=0)
            low_t[row] = jnp.concatenate(split(block.T), axis=0)
            rhs[row] = chunks[k, share + r]
            return carry

        copies[k].wait()
        lax.fori_loop(0, share, place, 0, unroll=True)
    to_left[0] = products([low_t[0]], side_by_side(rhs[0]))
    to_right[0] = rhs[per_dev - 1]


def unpack_diag(count, share, dest, weights, gate, *rest):
    arrived = rest[:count]
    diag, centre, chunks, sems = rest[count:]
    copies = [pltpu.make_async_copy(arrived[k], chunks.at[k], sems.at[k]) for k in range(count)]
    for copy in copies:
        copy.start()
    size = diag.shape[2]
    half = size // 2
    across = lax.broadcasted_iota(jnp.int32, (half, size), 1)
    down = lax.broadcasted_iota(jnp.int32, (half, size), 0)
    eye = lax.broadcasted_iota(jnp.int32, (size, size), 0) == lax.broadcasted_iota(jnp.int32, (size, size), 1)
    for k in range(count):
        copies[k].wait()
        for r in range(share):
            packed = chunks[k][r * half : (r + 1) * half, :]
            along = chunks[k][share * half + r : share * half + r + 1, :]
            top = jnp.where((across >= half) | (across > down), packed, 0.0)
            bottom = pltpu.roll(jnp.where(across < down, packed, 0.0), half, 1)
            above = jnp.concatenate([top, bottom], axis=0)
            block = jnp.where(eye, along, above + above.T)
            diag[dest[k * share + r]] = jnp.concatenate(split(block), axis=0)
    traces = jnp.concatenate(
        [chunks[k][share * half + share : share * half + share + 1, :] for k in range(count)], axis=0
    )
    mean = jnp.sum(jnp.sum(weights[...] * traces[None], axis=1), axis=1, keepdims=True)
    centre[...] = jnp.broadcast_to(mean, centre.shape)


def products(blocks, parts):
    size = parts.shape[1] // 2
    full = jnp.dot(jnp.concatenate(blocks, axis=1), parts, preferred_element_type=F32)
    return (full[size:, size:] + (full[:size, size:] + full[size:, :size])) + full[:size, :size]


def folded(a, b):
    return jnp.sum((a * b).reshape(a.shape[0] // 8, 8, a.shape[1]), axis=0)


def side_by_side(x):
    return jnp.concatenate(split(x), axis=1)


def hold(held, j, value):
    size = value.shape[0]
    start = (j + 1) * size
    at = pl.ds(start if isinstance(j, int) else pl.multiple_of(start, size), size)
    high, remainder = split(value)
    held[at, 0:size] = high
    held[at, size : 2 * size] = remainder


def kept(held, j, count, size):
    start = (j + 1) * size
    return held[pl.ds(start if isinstance(j, int) else pl.multiple_of(start, size), count * size), :]


def coupling(field, above, turned, low, low_t, out, held):
    per_dev, size = field.shape[0], field.shape[1]
    hold(held, -1, above[0])
    hold(held, 0, field[0])
    hold(held, 1, field[1])

    def body(j, carry):
        hold(held, j + 1, field[j + 1])
        parts = jnp.concatenate([kept(held, j - 1, 1, size), kept(held, j + 1, 1, size)], axis=0)
        out[j] = products([low[j], low_t[j + 1]], parts)
        return carry

    lax.fori_loop(0, per_dev - 1, body, 0, unroll=UNROLL)
    last = per_dev - 1
    out[last] = products([low[last]], kept(held, last - 1, 1, size)) + turned[0]


def advance(image, now, mean):
    return (image - mean * now) * (1.0 / mean)


def step_edge(first, field, diag, centre, *rest):
    if first:
        coupled, low_t, top, bottom, to_left = rest
    else:
        above, turned, low, low_t, top, bottom, to_left = rest
    last = field.shape[0] - 1
    if first:
        upper = products([diag[0]], side_by_side(field[0])) + coupled[0]
        lower = products([diag[last]], side_by_side(field[last])) + coupled[last]
    else:
        parts = jnp.concatenate([side_by_side(f) for f in (above[0], field[0], field[1])], axis=0)
        upper = products([low[0], diag[0], low_t[1]], parts)
        parts = jnp.concatenate([side_by_side(f) for f in (field[last - 1], field[last])], axis=0)
        lower = products([low[last], diag[last]], parts) + turned[0]
    new = advance(upper, field[0], centre[0:1, :])
    top[0] = new
    to_left[0] = products([low_t[0]], side_by_side(new))
    bottom[0] = advance(lower, field[last], centre[last : last + 1, :])


def step_inner(first, whole, seg, field, diag, centre, *rest):
    if first:
        coupled, edge_top, edge_bottom, out, table, held = rest
    elif whole:
        low, low_t, above, turned, out, table, held = rest
    else:
        low, low_t, edge_top, edge_bottom, out, table, held = rest
    per_dev, size = field.shape[0], field.shape[1]
    last = per_dev - 1
    table[...] = jnp.zeros(table.shape, F32)

    def sums(j, now, new):
        system = seg[j]
        table[system, 0] += folded(now, new)
        if not whole:
            table[system, 1] += folded(new, new)
        if first:
            table[system, 2] += folded(now, now)

    def one(j, image):
        now = field[j]
        new = advance(image, now, centre[pl.ds(j, 1), :])
        out[j] = new
        sums(j, now, new)

    def body(j, carry):
        if first:
            one(j, products([diag[j]], side_by_side(field[j])) + coupled[j])
        else:
            hold(held, j + 1, field[j + 1])
            one(j, products([low[j], diag[j], low_t[j + 1]], kept(held, j - 1, 3, size)))
        return carry

    if not first:
        hold(held, 0, field[0])
        hold(held, 1, field[1])
    if whole:
        hold(held, -1, above[0])
        one(0, products([low[0], diag[0], low_t[1]], kept(held, -1, 3, size)))
    else:
        out[0] = edge_top[0]
        sums(0, field[0], edge_top[0])
    lax.fori_loop(1, last, body, 0, unroll=UNROLL)
    if whole:
        one(last, products([low[last], diag[last]], kept(held, last - 1, 2, size)) + turned[0])
    else:
        out[last] = edge_bottom[0]
        sums(last, field[last], edge_bottom[0])


def gather_sums(tables_count, sends, *rest):
    tables, moments, messages = rest[:tables_count], rest[tables_count], rest[tables_count + 1 :]
    moments[0] = jnp.sum(tables[0][:, 2], axis=1)
    for i, table in enumerate(tables):
        for m in range(2 if i + 1 < tables_count else 1):
            moments[2 * i + 1 + m] = jnp.sum(table[:, m], axis=1)
    for i, message in enumerate(messages):
        for k in range(2 * tables_count):
            message[k : k + 1, :] = moments[k, pl.ds(sends[i], 1), :]


def finish(reach, seg, meets, moments, *rest):
    received = rest[: 2 * reach]
    bases = rest[2 * reach : 2 * reach + ITERS + 1]
    centre, sol, res, coef = rest[2 * reach + ITERS + 1 :]
    rows = sol.shape[0]
    systems = moments.shape[1]

    @pl.when(pl.program_id(0) == 0)
    def _():
        index = lax.broadcasted_iota(jnp.int32, (systems, moments.shape[2]), 0)
        m = []
        for k in range(2 * ITERS):
            total = moments[k]
            for i in range(2 * reach):
                total = total + jnp.where(index == meets[i], received[i][k : k + 1, :], 0.0)
            m.append(total)

        def inner(a, b):
            by_degree = {}
            for i, u in enumerate(a):
                for j, v in enumerate(b):
                    by_degree[i + j] = u * v if i + j not in by_degree else by_degree[i + j] + u * v
            return functools.reduce(lambda x, y: x + y, [w * m[d] for d, w in by_degree.items()])

        def ratio(a, b):
            good = (a > 0) & (b > 0)
            return jnp.where(good, a / jnp.where(good, b, 1.0), 0.0)

        one = jnp.ones_like(m[0])
        remains, along, summed = [one], [one], []
        norm = m[0]
        for step in range(ITERS):
            image = [along[0]] + [along[i] + along[i - 1] for i in range(1, len(along))] + [along[-1]]
            size = ratio(norm, inner(along, image))
            summed = [size * a + (summed[i] if i < len(summed) else 0.0) for i, a in enumerate(along)]
            remains = [(remains[i] if i < len(remains) else 0.0) - size * a for i, a in enumerate(image)]
            if step + 1 < ITERS:
                norm_next = inner(remains, remains)
                grow = ratio(norm_next, norm)
                along = [a + (grow * along[i] if i < len(along) else 0.0) for i, a in enumerate(remains)]
                norm = norm_next
        for i in range(ITERS):
            coef[i] = summed[i]
        for i in range(ITERS + 1):
            coef[ITERS + i] = remains[i]

    for j in range(rows):
        row = pl.program_id(0) * rows + j
        system = seg[row]
        values = [basis[j] for basis in bases]
        mean = centre[pl.ds(row, 1), :]
        pick = lambda i: coef[i, pl.ds(system, 1), :]
        inverse = 1.0 / mean
        sol[j] = functools.reduce(
            lambda x, y: x + y, [(pick(i) * inverse) * values[i] for i in reversed(range(ITERS))]
        )
        res[j] = functools.reduce(
            lambda x, y: x + y, [pick(ITERS + i) * values[i] for i in reversed(range(ITERS + 1))]
        )


def body(placing, lengths, diag_blocks, lower_blocks, right_side):
    count = lax.axis_size("row")
    device = lax.axis_index("row")
    per_dev, size = diag_blocks.shape[0], diag_blocks.shape[1]
    width = right_side.shape[2]
    share = per_dev // count
    systems = lengths.shape[0]
    total = count * per_dev
    reach = min(count - 1, -(-(MOSTLEN - 1) // per_dev))
    half = size // 2
    swaps = [(by, phase) for by in range(reach, 0, -1) for phase in range(2)]
    slots = jnp.arange(per_dev, dtype=jnp.int32)
    earlier = slots[None, :] < slots[:, None]

    coupled_shape = (2 * share, size, width)
    sent = call(
        functools.partial(pack_coupled, count, share),
        [sds(coupled_shape)] * count + [sds((per_dev,), jnp.int32)],
        [SMEM, HBM, HBM],
        [VMEM] * count + [SMEM],
        [pltpu.SMEM((count,), jnp.int32), pltpu.SemaphoreType.DMA((2 * per_dev,))],
        name="pack_coupled",
    )(placing, in_hbm(lower_blocks), in_hbm(right_side))
    order = sent[count]
    coupled = [sent[0]] + [shifted(sent[k], k) for k in range(1, count)]

    ends = jnp.cumsum(lengths)

    def system_of(rows):
        return jnp.sum((rows[..., None] >= ends).astype(jnp.int32), axis=-1)

    row0 = device * per_dev
    rows = row0 + slots
    seg = system_of(rows)
    keep = (seg != system_of(rows - 1)) | (rows == 0)
    keep = 1 - keep.astype(jnp.int32)
    first_system, last_system = seg[0], seg[per_dev - 1]
    meets, sends = [], []
    for by, phase in swaps:
        onward = (device // by + phase) % 2 == 0
        row = jnp.where(onward, row0 + by * per_dev, row0 - (by - 1) * per_dev - 1)
        mine = jnp.where(onward, last_system, first_system)
        meets.append(jnp.where((row >= 0) & (row < total) & (system_of(row) == mine), mine, -1))
        sends.append(mine)
    meets, sends = jnp.stack(meets), jnp.stack(sends)

    table = placing.reshape(count, per_dev)[::-1]
    table = lax.dynamic_slice_in_dim(jnp.concatenate([table, table]), count - 1 - device, count)
    mine = table // per_dev == device
    rank = jnp.sum((earlier[None] & mine[:, None, :]).astype(jnp.int32), axis=2)
    picks = mine[:, None, :] & (rank[:, None, :] == jnp.arange(share, dtype=jnp.int32)[None, :, None])
    dest = jnp.sum(jnp.where(picks, table[:, None, :] - row0, 0), axis=2).reshape(-1)
    in_length = jnp.sum(jnp.where(seg[:, None] == jnp.arange(systems)[None, :], lengths[None, :], 0), axis=1)
    weights = jnp.where(
        seg[:, None, None] == system_of(table)[None], 1.0 / (size * in_length.astype(F32))[:, None, None], 0.0
    )
    weights = jnp.pad(weights, ((0, 0), (0, 0), (0, size - per_dev)))

    order, seg, keep, sends, meets, dest, weights = lax.optimization_barrier(
        (order, seg, keep, sends, meets, dest, weights)
    )

    diag_rows = share * half + 8 * (-(-(share + 1) // 8))
    sent = call(
        functools.partial(pack_diag, count, share),
        [sds((diag_rows, size))] * count,
        [SMEM, HBM, ANY],
        [VMEM] * count,
        [pltpu.VMEM((per_dev, size, size), F32), pltpu.SemaphoreType.DMA((per_dev,))],
        name="pack_diag",
    )(order, in_hbm(diag_blocks), coupled[GATE])
    halves = [sent[0]] + [shifted(sent[k], k) for k in range(1, count)]

    field_shape, row_shape = sds((per_dev, size, width)), sds((1, size, width))
    block_shape = sds((per_dev, 2 * size, size), BF16)
    rhs, low, low_t, to_left, to_right = call(
        functools.partial(unpack_coupled, count, share),
        [field_shape, block_shape, block_shape, row_shape, row_shape],
        [SMEM, SMEM] + [ANY] * count,
        [VMEM] * 5,
        [pltpu.VMEM((count,) + coupled_shape, F32), pltpu.SemaphoreType.DMA((count,))],
        name="unpack_coupled",
    )(dest, keep, *coupled)
    turned = shifted(to_left, -1)
    above = shifted(to_right, 1)
    held = [pltpu.VMEM(((per_dev + 2) * size, 2 * width), BF16)]
    partly = call(
        coupling, field_shape, [VMEM] * 5, VMEM, held, flops=300000000, name="coupling"
    )(rhs, above, turned, low, low_t)

    diag, centre = call(
        functools.partial(unpack_diag, count, share),
        [block_shape, sds((per_dev, width))],
        [SMEM, VMEM, ANY] + [ANY] * count,
        [VMEM] * 2,
        [pltpu.VMEM((count, diag_rows, size), F32), pltpu.SemaphoreType.DMA((count,))],
        name="unpack_diag",
    )(dest, weights, partly, *halves)

    bases, tables = [rhs], []
    for i in range(ITERS):
        field = bases[-1]
        first, whole = i == 0, i + 1 == ITERS
        common = (field, diag, centre)
        if not whole:
            extra = (partly, low_t) if first else (above, turned, low, low_t)
            top, bottom, to_left = call(
                functools.partial(step_edge, first),
                [row_shape] * 3,
                [VMEM] * (3 + len(extra)),
                [VMEM] * 3,
                name="step_edge",
            )(*common, *extra)
        if first:
            extra = (partly, top, bottom)
        elif whole:
            extra = (low, low_t, above, turned)
        else:
            extra = (low, low_t, top, bottom)
        new, sums = call(
            functools.partial(step_inner, first, whole),
            [field_shape, sds((systems, 3 if first else 2, 8, width))],
            [SMEM] + [VMEM] * (3 + len(extra)),
            [VMEM] * 2,
            held,
            flops=400000000,
            name="step_inner",
        )(seg, *common, *extra)
        if not whole:
            above = shifted(bottom, 1)
            turned = shifted(to_left, -1)
        bases.append(new)
        tables.append(sums)

    moments, *messages = call(
        functools.partial(gather_sums, ITERS),
        [sds((2 * ITERS, systems, width))] + [sds((2 * ITERS, width))] * len(swaps),
        [SMEM] + [VMEM] * ITERS,
        [VMEM] * (1 + len(swaps)),
        name="gather_sums",
    )(sends, *tables)
    received = [swapped(message, *swap) for message, swap in zip(messages, swaps)]

    step = 4 if per_dev % 4 == 0 else 1
    block = pl.BlockSpec((step, size, width), lambda i: (i, 0, 0))
    return pl.pallas_call(
        functools.partial(finish, reach),
        out_shape=[field_shape] * 2,
        grid=(per_dev // step,),
        in_specs=[SMEM, SMEM, VMEM] + [VMEM] * (2 * reach) + [block] * (ITERS + 1) + [VMEM],
        out_specs=[block] * 2,
        scratch_shapes=[pltpu.VMEM((2 * ITERS + 1, systems, width), F32)],
        compiler_params=pltpu.CompilerParams(vmem_limit_bytes=20 * MIB),
        name="finish",
    )(seg, meets, moments, *received, *bases, centre)


def solution(mesh):
    spec = P(("grp", "row"), None, None)
    return jax.shard_map(
        lambda *args: tuple(body(*args)),
        mesh=mesh,
        in_specs=(P("grp"), P("grp"), spec, spec, spec),
        out_specs=(spec, spec),
        check_vma=False,
    )
```

```python
import functools
import math

import jax
import jax.numpy as jnp
from jax import lax
from jax.experimental import pallas as pl
from jax.experimental.pallas import tpu as pltpu
from jax.sharding import PartitionSpec as P

ITERS = 4
MOSTLEN = 48


F32 = jnp.float32
BF16 = jnp.bfloat16
ANY = pl.BlockSpec(memory_space=pl.ANY)
VMEM = pl.BlockSpec(memory_space=pltpu.VMEM)
SMEM = pl.BlockSpec(memory_space=pltpu.SMEM)
HBM = pl.BlockSpec(memory_space=pltpu.HBM)
MIB = 1 << 20
GATE = 0
UNROLL = True


def shifted(x, by):
    count = lax.axis_size("row")
    return lax.ppermute(x, "row", [(i, (i + by) % count) for i in range(count)])


def sds(shape, dtype=F32):
    return jax.ShapeDtypeStruct(shape, dtype)


def in_hbm(x):
    return pltpu.with_memory_space_constraint(x, pltpu.HBM)


def call(kernel, out_shape, in_specs, out_specs, scratch=(), vmem=20, flops=1000000, **extra):
    return pl.pallas_call(
        kernel,
        out_shape=out_shape,
        in_specs=in_specs,
        out_specs=out_specs,
        scratch_shapes=list(scratch),
        compiler_params=pltpu.CompilerParams(vmem_limit_bytes=vmem * MIB),
        cost_estimate=pl.CostEstimate(flops=flops, transcendentals=0, bytes_accessed=0),
        **extra,
    )


def split(x):
    high = x.astype(BF16)
    return high, (x - high.astype(F32)).astype(BF16)


def quotient(x, by):
    return lax.shift_right_logical(x, jnp.int32(by.bit_length() - 1)) if by & (by - 1) == 0 else lax.div(x, by)


def remainder(x, by):
    return x & (by - 1) if by & (by - 1) == 0 else lax.rem(x, by)


def ranked(count, share, placing, order, seen):
    device = lax.axis_index("row")
    per_dev = count * share
    base = device * per_dev
    for k in range(count):
        seen[k] = 0

    def rank(s, carry):
        target = quotient(placing[base + s], per_dev)
        k = remainder(target - device + count, count)
        order[k * share + seen[k]] = s
        seen[k] = seen[k] + 1
        return carry

    lax.fori_loop(0, per_dev, rank, 0, unroll=True)


def pack_coupled(count, share, placing, lower, rhs, *rest):
    outs, (order, seen, chunks, sems, out_sems) = rest[:count], rest[count:]
    ranked(count, share, placing, order, seen)
    for k in range(count):
        for r in range(share):
            slot = order[k * share + r]
            pltpu.make_async_copy(lower.at[slot], chunks.at[k, r], sems.at[k]).start()
            pltpu.make_async_copy(rhs.at[slot], chunks.at[k, share + r], sems.at[k]).start()
    leaving = [pltpu.make_async_copy(chunks.at[k], outs[k], out_sems.at[k]) for k in range(count)]
    for k in range(count):
        pltpu.make_async_copy(lower.at[pl.ds(0, 2 * share)], chunks.at[k], sems.at[k]).wait()
        leaving[k].start()
    for copy in leaving:
        copy.wait()


def pack_diag(count, share, order, diag, gate, *rest):
    outs, held, sems = rest[:count], rest[count], rest[count + 1]
    size = diag.shape[1]
    half = size // 2
    per_dev = count * share

    def fetch(q):
        return pltpu.make_async_copy(diag.at[order[q]], held.at[q], sems.at[q])

    for q in range(per_dev):
        fetch(q).start()
    across = lax.broadcasted_iota(jnp.int32, (half, size), 1)
    down = lax.broadcasted_iota(jnp.int32, (half, size), 0)
    eye = lax.broadcasted_iota(jnp.int32, (size, size), 0) == lax.broadcasted_iota(jnp.int32, (size, size), 1)
    lane = lax.broadcasted_iota(jnp.int32, (1, size), 1)
    traces = jnp.zeros((1, size), F32)
    for k in range(count):
        for r in range(share):
            q = k * share + r
            fetch(q).wait()
            block = held[q]
            top, turned = block[:half], pltpu.roll(block[half:], half, 1)
            outs[k][r * half : (r + 1) * half, :] = jnp.where(
                across >= half, top, jnp.where(across > down, top, turned)
            )
            along = jnp.sum(jnp.where(eye, block, 0.0), axis=0, keepdims=True)
            outs[k][share * half + r : share * half + r + 1, :] = along
            traces = jnp.where(lane == order[q], jnp.sum(along, axis=1, keepdims=True), traces)
    for k in range(count):
        outs[k][share * half + share : share * half + share + 1, :] = traces


def unpack_coupled(count, share, dest, keep, *rest):
    arrived = rest[:count]
    rhs, low, low_t, to_left, to_right, chunks, sems = rest[count:]
    per_dev = rhs.shape[0]
    copies = [pltpu.make_async_copy(arrived[k], chunks.at[k], sems.at[k]) for k in range(count)]
    for copy in copies:
        copy.start()
    for k in range(count):

        def place(r, carry, k=k):
            row = dest[k * share + r]
            block = jnp.where(keep[row] > 0, chunks[k, r], 0.0)
            low[row] = jnp.concatenate(split(block), axis=0)
            low_t[row] = jnp.concatenate(split(block.T), axis=0)
            rhs[row] = chunks[k, share + r]
            return carry

        copies[k].wait()
        lax.fori_loop(0, share, place, 0, unroll=True)
    to_left[0] = products([low_t[0]], side_by_side(rhs[0]))
    to_right[0] = rhs[per_dev - 1]


def unpack_diag(share, near, far, dest, *rest):
    group = near if far is None else far
    if far is not None:
        weights, others, other_traces = rest[:3]
        rest = rest[3:]
    arrived = rest[: len(group)]
    diag, out, chunks, sems = rest[-4:]
    copies = [pltpu.make_async_copy(arrived[i], chunks.at[i], sems.at[i]) for i in range(len(group))]
    for copy in copies:
        copy.start()
    size = diag.shape[2]
    half = size // 2
    across = lax.broadcasted_iota(jnp.int32, (half, size), 1)
    down = lax.broadcasted_iota(jnp.int32, (half, size), 0)
    eye = lax.broadcasted_iota(jnp.int32, (size, size), 0) == lax.broadcasted_iota(jnp.int32, (size, size), 1)
    if far is not None:
        diag[...] = others[...]
    traces = {}
    for i, k in enumerate(group):
        copies[i].wait()
        for r in range(share):
            packed = chunks[i, r * half : (r + 1) * half, :]
            along = chunks[i, share * half + r : share * half + r + 1, :]
            top = jnp.where((across >= half) | (across > down), packed, 0.0)
            bottom = pltpu.roll(jnp.where(across < down, packed, 0.0), half, 1)
            above = jnp.concatenate([top, bottom], axis=0)
            block = jnp.where(eye, along, above + above.T)
            diag[dest[k * share + r]] = jnp.concatenate(split(block), axis=0)
        traces[k] = chunks[i, share * half + share : share * half + share + 1, :]
    if far is None:
        for i, k in enumerate(group):
            out[i : i + 1, :] = traces[k]
    else:
        for i, k in enumerate(near):
            traces[k] = other_traces[i : i + 1, :]
        rows = jnp.concatenate([traces[k] for k in range(len(traces))], axis=0)
        mean = jnp.sum(jnp.sum(weights[...] * rows[None], axis=1), axis=1, keepdims=True)
        out[...] = jnp.broadcast_to(mean, out.shape)


def products(blocks, parts):
    size = parts.shape[1] // 2
    full = jnp.dot(jnp.concatenate(blocks, axis=1), parts, preferred_element_type=F32)
    return (full[size:, size:] + (full[:size, size:] + full[size:, :size])) + full[:size, :size]


def folded(a, b):
    return jnp.sum((a * b).reshape(a.shape[0] // 8, 8, a.shape[1]), axis=0)


def side_by_side(x):
    return jnp.concatenate(split(x), axis=1)


def hold(held, j, value):
    size = value.shape[0]
    start = (j + 1) * size
    at = pl.ds(start if isinstance(j, int) else pl.multiple_of(start, size), size)
    high, remainder = split(value)
    held[at, 0:size] = high
    held[at, size : 2 * size] = remainder


def kept(held, j, count, size):
    start = (j + 1) * size
    return held[pl.ds(start if isinstance(j, int) else pl.multiple_of(start, size), count * size), :]


def coupling(field, low, low_t, out, held):
    per_dev, size = field.shape[0], field.shape[1]
    last = per_dev - 1
    hold(held, 0, field[0])
    hold(held, 1, field[1])
    out[0] = products([low_t[1]], kept(held, 1, 1, size))

    def body(j, carry):
        hold(held, j + 1, field[j + 1])
        parts = jnp.concatenate([kept(held, j - 1, 1, size), kept(held, j + 1, 1, size)], axis=0)
        out[j] = products([low[j], low_t[j + 1]], parts)
        return carry

    lax.fori_loop(1, last, body, 0, unroll=UNROLL)
    out[last] = products([low[last]], kept(held, last - 1, 1, size))


def advance(image, now, mean):
    return (image - mean * now) * (1.0 / mean)


def step_edge(first, field, diag, centre, *rest):
    above, turned, low, low_t = rest[:4]
    top, bottom, to_left = rest[-3:]
    last = field.shape[0] - 1
    if first:
        coupled = rest[4]
        parts = jnp.concatenate([side_by_side(f) for f in (above[0], field[0])], axis=0)
        upper = products([low[0], diag[0]], parts) + coupled[0]
        lower = products([diag[last]], side_by_side(field[last])) + coupled[last] + turned[0]
    else:
        parts = jnp.concatenate([side_by_side(f) for f in (above[0], field[0], field[1])], axis=0)
        upper = products([low[0], diag[0], low_t[1]], parts)
        parts = jnp.concatenate([side_by_side(f) for f in (field[last - 1], field[last])], axis=0)
        lower = products([low[last], diag[last]], parts) + turned[0]
    new = advance(upper, field[0], centre[0:1, :])
    top[0] = new
    to_left[0] = products([low_t[0]], side_by_side(new))
    bottom[0] = advance(lower, field[last], centre[last : last + 1, :])


def step_inner(first, whole, seg, field, diag, centre, *rest):
    if first:
        coupled, edge_top, edge_bottom, out, table, held = rest
    elif whole:
        low, low_t, above, turned, out, table, held = rest
    else:
        low, low_t, edge_top, edge_bottom, out, table, held = rest
    per_dev, size = field.shape[0], field.shape[1]
    last = per_dev - 1
    table[...] = jnp.zeros(table.shape, F32)

    def sums(j, now, new):
        system = seg[j]
        table[system, 0] += folded(now, new)
        if not whole:
            table[system, 1] += folded(new, new)
        if first:
            table[system, 2] += folded(now, now)

    def one(j, image):
        now = field[j]
        new = advance(image, now, centre[pl.ds(j, 1), :])
        out[j] = new
        sums(j, now, new)

    def body(j, carry):
        if first:
            one(j, products([diag[j]], side_by_side(field[j])) + coupled[j])
        else:
            hold(held, j + 1, field[j + 1])
            one(j, products([low[j], diag[j], low_t[j + 1]], kept(held, j - 1, 3, size)))
        return carry

    if not first:
        hold(held, 0, field[0])
        hold(held, 1, field[1])
    if whole:
        hold(held, -1, above[0])
        one(0, products([low[0], diag[0], low_t[1]], kept(held, -1, 3, size)))
    else:
        out[0] = edge_top[0]
        sums(0, field[0], edge_top[0])
    lax.fori_loop(1, last, body, 0, unroll=UNROLL)
    if whole:
        one(last, products([low[last], diag[last]], kept(held, last - 1, 2, size)) + turned[0])
    else:
        out[last] = edge_bottom[0]
        sums(last, field[last], edge_bottom[0])


def gather_sums(tables_count, sends, *rest):
    tables, moments, messages = rest[:tables_count], rest[tables_count], rest[tables_count + 1 :]
    moments[0] = jnp.sum(tables[0][:, 2], axis=1)
    for i, table in enumerate(tables):
        for m in range(2 if i + 1 < tables_count else 1):
            moments[2 * i + 1 + m] = jnp.sum(table[:, m], axis=1)
    for i, message in enumerate(messages):
        for k in range(2 * tables_count):
            message[k : k + 1, :] = moments[k, pl.ds(sends[i], 1), :]


def finish(reach, seg, meets, moments, *rest):
    received = rest[: 2 * reach]
    bases = rest[2 * reach : 2 * reach + ITERS + 1]
    centre, sol, res, coef = rest[2 * reach + ITERS + 1 :]
    rows = sol.shape[0]
    systems = moments.shape[1]

    @pl.when(pl.program_id(0) == 0)
    def _():
        index = lax.broadcasted_iota(jnp.int32, (systems, moments.shape[2]), 0)
        m = []
        for k in range(2 * ITERS):
            total = moments[k]
            for i in range(2 * reach):
                total = total + jnp.where(index == meets[i], received[i][k : k + 1, :], 0.0)
            m.append(total)

        def inner(a, b):
            by_degree = {}
            for i, u in enumerate(a):
                for j, v in enumerate(b):
                    by_degree[i + j] = u * v if i + j not in by_degree else by_degree[i + j] + u * v
            return functools.reduce(lambda x, y: x + y, [w * m[d] for d, w in by_degree.items()])

        def ratio(a, b):
            good = (a > 0) & (b > 0)
            return jnp.where(good, a / jnp.where(good, b, 1.0), 0.0)

        one = jnp.ones_like(m[0])
        remains, along, summed = [one], [one], []
        norm = m[0]
        for step in range(ITERS):
            image = [along[0]] + [along[i] + along[i - 1] for i in range(1, len(along))] + [along[-1]]
            size = ratio(norm, inner(along, image))
            summed = [size * a + (summed[i] if i < len(summed) else 0.0) for i, a in enumerate(along)]
            remains = [(remains[i] if i < len(remains) else 0.0) - size * a for i, a in enumerate(image)]
            if step + 1 < ITERS:
                norm_next = inner(remains, remains)
                grow = ratio(norm_next, norm)
                along = [a + (grow * along[i] if i < len(along) else 0.0) for i, a in enumerate(remains)]
                norm = norm_next
        for i in range(ITERS):
            coef[i] = summed[i]
        for i in range(ITERS + 1):
            coef[ITERS + i] = remains[i]

    for j in range(rows):
        row = pl.program_id(0) * rows + j
        system = seg[row]
        values = [basis[j] for basis in bases]
        mean = centre[pl.ds(row, 1), :]
        pick = lambda i: coef[i, pl.ds(system, 1), :]
        inverse = 1.0 / mean
        sol[j] = functools.reduce(
            lambda x, y: x + y, [(pick(i) * inverse) * values[i] for i in reversed(range(ITERS))]
        )
        res[j] = functools.reduce(
            lambda x, y: x + y, [pick(ITERS + i) * values[i] for i in reversed(range(ITERS + 1))]
        )


def body(placing, lengths, diag_blocks, lower_blocks, right_side):
    count = lax.axis_size("row")
    device = lax.axis_index("row")
    per_dev, size = diag_blocks.shape[0], diag_blocks.shape[1]
    width = right_side.shape[2]
    share = per_dev // count
    systems = lengths.shape[0]
    total = count * per_dev
    reach = min(count - 1, -(-(MOSTLEN - 1) // per_dev))
    half = size // 2
    swaps = [1, -1, 2, -2]
    slots = jnp.arange(per_dev, dtype=jnp.int32)
    earlier = slots[None, :] < slots[:, None]

    distances = sorted(range(1, count), key=lambda k: -min(k, count - k))
    far = [k for k in distances if 4 * min(k, count - k) > count]
    near = [0] + [k for k in distances if k not in far]
    coupled_shape = (2 * share, size, width)
    coupled = [None] * count
    *sent, order = call(
        functools.partial(pack_coupled, count, share),
        [sds(coupled_shape)] * count + [sds((per_dev,), jnp.int32)],
        [SMEM, HBM, HBM],
        [HBM] * count + [SMEM],
        [
            pltpu.SMEM((count,), jnp.int32),
            pltpu.VMEM((count,) + coupled_shape, F32),
            pltpu.SemaphoreType.DMA((count,)),
            pltpu.SemaphoreType.DMA((count,)),
        ],
        name="pack_coupled",
    )(placing, in_hbm(lower_blocks), in_hbm(right_side))
    coupled[0] = sent[0]
    for k in distances:
        coupled[k] = shifted(sent[k], k)

    ends = jnp.cumsum(lengths)

    def system_of(rows):
        return jnp.sum((rows[..., None] >= ends).astype(jnp.int32), axis=-1)

    row0 = device * per_dev
    rows = row0 + slots
    seg = system_of(rows)
    keep = (seg != system_of(rows - 1)) | (rows == 0)
    keep = 1 - keep.astype(jnp.int32)
    first_system, last_system = seg[0], seg[per_dev - 1]
    meets, sends = [], []
    for by in swaps:
        row = row0 - (by - 1) * per_dev - 1 if by > 0 else row0 - by * per_dev
        mine = first_system if by > 0 else last_system
        meets.append(jnp.where((row >= 0) & (row < total) & (system_of(row) == mine), mine, -1))
        sends.append(last_system if by > 0 else first_system)
    meets, sends = jnp.stack(meets), jnp.stack(sends)

    table = placing.reshape(count, per_dev)[::-1]
    table = lax.dynamic_slice_in_dim(jnp.concatenate([table, table]), count - 1 - device, count)
    mine = table // per_dev == device
    rank = jnp.sum((earlier[None] & mine[:, None, :]).astype(jnp.int32), axis=2)
    picks = mine[:, None, :] & (rank[:, None, :] == jnp.arange(share, dtype=jnp.int32)[None, :, None])
    dest = jnp.sum(jnp.where(picks, table[:, None, :] - row0, 0), axis=2).reshape(-1)
    in_length = jnp.sum(jnp.where(seg[:, None] == jnp.arange(systems)[None, :], lengths[None, :], 0), axis=1)
    weights = jnp.where(
        seg[:, None, None] == system_of(table)[None], 1.0 / (size * in_length.astype(F32))[:, None, None], 0.0
    )
    weights = jnp.pad(weights, ((0, 0), (0, 0), (0, size - per_dev)))

    order, seg, keep, sends, meets, dest, weights = lax.optimization_barrier(
        (order, seg, keep, sends, meets, dest, weights)
    )

    diag_rows = share * half + 8 * (-(-(share + 1) // 8))
    sent = call(
        functools.partial(pack_diag, count, share),
        [sds((diag_rows, size))] * count,
        [SMEM, HBM, ANY],
        [VMEM] * count,
        [pltpu.VMEM((per_dev, size, size), F32), pltpu.SemaphoreType.DMA((per_dev,))],
        name="pack_diag",
    )(order, in_hbm(diag_blocks), coupled[GATE])
    halves = [sent[0]] + [None] * (count - 1)
    for k in distances:
        halves[k] = shifted(sent[k], k)

    field_shape, row_shape = sds((per_dev, size, width)), sds((1, size, width))
    block_shape = sds((per_dev, 2 * size, size), BF16)
    rhs, low, low_t, to_left, to_right = call(
        functools.partial(unpack_coupled, count, share),
        [field_shape, block_shape, block_shape, row_shape, row_shape],
        [SMEM, SMEM] + [ANY] * count,
        [VMEM] * 5,
        [pltpu.VMEM((count,) + coupled_shape, F32), pltpu.SemaphoreType.DMA((count,))],
        name="unpack_coupled",
    )(dest, keep, *coupled)
    turned = shifted(to_left, -1)
    above = shifted(to_right, 1)
    held = [pltpu.VMEM(((per_dev + 2) * size, 2 * width), BF16)]
    partly = call(
        coupling, field_shape, [VMEM] * 3, VMEM, held, flops=300000000, name="coupling"
    )(rhs, low, low_t)

    near_diag = call(
        functools.partial(unpack_diag, share, near, None),
        [block_shape, sds((len(near), size))],
        [SMEM] + [ANY] * len(near) + [ANY],
        [VMEM] * 2,
        [pltpu.VMEM((len(near), diag_rows, size), F32), pltpu.SemaphoreType.DMA((len(near),))],
        name="unpack_diag_near",
    )(dest, *[halves[k] for k in near], partly)
    diag, centre = call(
        functools.partial(unpack_diag, share, near, far),
        [block_shape, sds((per_dev, width))],
        [SMEM, VMEM, VMEM, VMEM] + [ANY] * len(far),
        [VMEM] * 2,
        [pltpu.VMEM((len(far), diag_rows, size), F32), pltpu.SemaphoreType.DMA((len(far),))],
        name="unpack_diag_far",
    )(dest, weights, *near_diag, *[halves[k] for k in far])

    bases, tables = [rhs], []
    for i in range(ITERS):
        field = bases[-1]
        first, whole = i == 0, i + 1 == ITERS
        common = (field, diag, centre)
        if not whole:
            extra = (above, turned, low, low_t) + ((partly,) if first else ())
            top, bottom, to_left = call(
                functools.partial(step_edge, first),
                [row_shape] * 3,
                [VMEM] * (3 + len(extra)),
                [VMEM] * 3,
                name="step_edge",
            )(*common, *extra)
        if first:
            extra = (partly, top, bottom)
        elif whole:
            extra = (low, low_t, above, turned)
        else:
            extra = (low, low_t, top, bottom)
        new, sums = call(
            functools.partial(step_inner, first, whole),
            [field_shape, sds((systems, 3 if first else 2, 8, width))],
            [SMEM] + [VMEM] * (3 + len(extra)),
            [VMEM] * 2,
            held,
            flops=400000000,
            name="step_inner",
        )(seg, *common, *extra)
        if not whole:
            above = shifted(bottom, 1)
            turned = shifted(to_left, -1)
        bases.append(new)
        tables.append(sums)

    moments, *messages = call(
        functools.partial(gather_sums, ITERS),
        [sds((2 * ITERS, systems, width))] + [sds((2 * ITERS, width))] * len(swaps),
        [SMEM] + [VMEM] * ITERS,
        [VMEM] * (1 + len(swaps)),
        name="gather_sums",
    )(sends, *tables)
    received = [shifted(message, swap) for message, swap in zip(messages, swaps)]

    step = math.gcd(per_dev, 8)
    block = pl.BlockSpec((step, size, width), lambda i: (i, 0, 0))
    return pl.pallas_call(
        functools.partial(finish, reach),
        out_shape=[field_shape] * 2,
        grid=(per_dev // step,),
        in_specs=[SMEM, SMEM, VMEM] + [VMEM] * (2 * reach) + [block] * (ITERS + 1) + [VMEM],
        out_specs=[block] * 2,
        scratch_shapes=[pltpu.VMEM((2 * ITERS + 1, systems, width), F32)],
        compiler_params=pltpu.CompilerParams(vmem_limit_bytes=20 * MIB),
        name="finish",
    )(seg, meets, moments, *received, *bases, centre)


def solution(mesh):
    spec = P(("grp", "row"), None, None)
    return jax.shard_map(
        lambda *args: tuple(body(*args)),
        mesh=mesh,
        in_specs=(P("grp"), P("grp"), spec, spec, spec),
        out_specs=(spec, spec),
        check_vma=False,
    )
```

```python
import functools
import math

import jax
import jax.numpy as jnp
from jax import lax
from jax.experimental import pallas as pl
from jax.experimental.pallas import tpu as pltpu
from jax.sharding import PartitionSpec as P

ITERS = 4
MOSTLEN = 48


F32 = jnp.float32
BF16 = jnp.bfloat16
ANY = pl.BlockSpec(memory_space=pl.ANY)
VMEM = pl.BlockSpec(memory_space=pltpu.VMEM)
SMEM = pl.BlockSpec(memory_space=pltpu.SMEM)
HBM = pl.BlockSpec(memory_space=pltpu.HBM)
MIB = 1 << 20
GATE = 0
UNROLL = True


def shifted(x, by):
    count = lax.axis_size("row")
    return lax.ppermute(x, "row", [(i, (i + by) % count) for i in range(count)])


def sds(shape, dtype=F32):
    return jax.ShapeDtypeStruct(shape, dtype)


def in_hbm(x):
    return pltpu.with_memory_space_constraint(x, pltpu.HBM)


def call(kernel, out_shape, in_specs, out_specs, scratch=(), vmem=20, flops=1000000, **extra):
    return pl.pallas_call(
        kernel,
        out_shape=out_shape,
        in_specs=in_specs,
        out_specs=out_specs,
        scratch_shapes=list(scratch),
        compiler_params=pltpu.CompilerParams(vmem_limit_bytes=vmem * MIB),
        cost_estimate=pl.CostEstimate(flops=flops, transcendentals=0, bytes_accessed=0),
        **extra,
    )


def split(x):
    high = x.astype(BF16)
    return high, (x - high.astype(F32)).astype(BF16)


def quotient(x, by):
    return lax.shift_right_logical(x, jnp.int32(by.bit_length() - 1)) if by & (by - 1) == 0 else lax.div(x, by)


def remainder(x, by):
    return x & (by - 1) if by & (by - 1) == 0 else lax.rem(x, by)


def ranked(count, share, placing, order, seen):
    device = lax.axis_index("row")
    per_dev = count * share
    base = device * per_dev
    for k in range(count):
        seen[k] = 0

    def rank(s, carry):
        target = quotient(placing[base + s], per_dev)
        k = remainder(target - device + count, count)
        order[k * share + seen[k]] = s
        seen[k] = seen[k] + 1
        return carry

    lax.fori_loop(0, per_dev, rank, 0, unroll=True)


def pack_coupled(count, share, placing, lower, rhs, *rest):
    outs, (order, seen, chunks, sems, out_sems) = rest[:count], rest[count:]
    ranked(count, share, placing, order, seen)
    by_reach = sorted(range(count), key=lambda k: -min(k, count - k))
    for k in by_reach:
        for r in range(share):
            slot = order[k * share + r]
            pltpu.make_async_copy(lower.at[slot], chunks.at[k, r], sems.at[k]).start()
            pltpu.make_async_copy(rhs.at[slot], chunks.at[k, share + r], sems.at[k]).start()
    leaving = [pltpu.make_async_copy(chunks.at[k], outs[k], out_sems.at[k]) for k in range(count)]
    for k in by_reach:
        pltpu.make_async_copy(lower.at[pl.ds(0, 2 * share)], chunks.at[k], sems.at[k]).wait()
        leaving[k].start()
    for copy in leaving:
        copy.wait()


def pack_diag(count, share, order, diag, gate, *rest):
    outs, held, sems = rest[:count], rest[count], rest[count + 1]
    size = diag.shape[1]
    half = size // 2
    per_dev = count * share

    def fetch(q):
        return pltpu.make_async_copy(diag.at[order[q]], held.at[q], sems.at[q])

    for q in range(per_dev):
        fetch(q).start()
    across = lax.broadcasted_iota(jnp.int32, (half, size), 1)
    down = lax.broadcasted_iota(jnp.int32, (half, size), 0)
    eye = lax.broadcasted_iota(jnp.int32, (size, size), 0) == lax.broadcasted_iota(jnp.int32, (size, size), 1)
    lane = lax.broadcasted_iota(jnp.int32, (1, size), 1)
    traces = jnp.zeros((1, size), F32)
    for k in range(count):
        for r in range(share):
            q = k * share + r
            fetch(q).wait()
            block = held[q]
            top, turned = block[:half], pltpu.roll(block[half:], half, 1)
            outs[k][r * half : (r + 1) * half, :] = jnp.where(
                across >= half, top, jnp.where(across > down, top, turned)
            )
            along = jnp.sum(jnp.where(eye, block, 0.0), axis=0, keepdims=True)
            outs[k][share * half + r : share * half + r + 1, :] = along
            traces = jnp.where(lane == order[q], jnp.sum(along, axis=1, keepdims=True), traces)
    for k in range(count):
        outs[k][share * half + share : share * half + share + 1, :] = traces


def unpack_coupled(count, share, dest, keep, *rest):
    arrived = rest[:count]
    rhs, low, low_t, to_left, to_right, chunks, sems = rest[count:]
    per_dev = rhs.shape[0]
    copies = [pltpu.make_async_copy(arrived[k], chunks.at[k], sems.at[k]) for k in range(count)]
    for copy in copies:
        copy.start()
    for k in range(count):

        def place(r, carry, k=k):
            row = dest[k * share + r]
            block = jnp.where(keep[row] > 0, chunks[k, r], 0.0)
            low[row] = jnp.concatenate(split(block), axis=0)
            low_t[row] = jnp.concatenate(split(block.T), axis=0)
            rhs[row] = chunks[k, share + r]
            return carry

        copies[k].wait()
        lax.fori_loop(0, share, place, 0, unroll=True)
    to_left[0] = products([low_t[0]], side_by_side(rhs[0]))
    to_right[0] = rhs[per_dev - 1]


def unpack_diag(share, near, far, dest, *rest):
    group = near if far is None else far
    if far is not None:
        weights, others, other_traces = rest[:3]
        rest = rest[3:]
    arrived = rest[: len(group)]
    diag, out, chunks, sems = rest[-4:]
    copies = [pltpu.make_async_copy(arrived[i], chunks.at[i], sems.at[i]) for i in range(len(group))]
    for copy in copies:
        copy.start()
    size = diag.shape[2]
    half = size // 2
    across = lax.broadcasted_iota(jnp.int32, (half, size), 1)
    down = lax.broadcasted_iota(jnp.int32, (half, size), 0)
    eye = lax.broadcasted_iota(jnp.int32, (size, size), 0) == lax.broadcasted_iota(jnp.int32, (size, size), 1)
    if far is not None:
        diag[...] = others[...]
    traces = {}
    for i, k in enumerate(group):
        copies[i].wait()
        for r in range(share):
            packed = chunks[i, r * half : (r + 1) * half, :]
            along = chunks[i, share * half + r : share * half + r + 1, :]
            top = jnp.where((across >= half) | (across > down), packed, 0.0)
            bottom = pltpu.roll(jnp.where(across < down, packed, 0.0), half, 1)
            above = jnp.concatenate([top, bottom], axis=0)
            block = jnp.where(eye, along, above + above.T)
            diag[dest[k * share + r]] = jnp.concatenate(split(block), axis=0)
        traces[k] = chunks[i, share * half + share : share * half + share + 1, :]
    if far is None:
        for i, k in enumerate(group):
            out[i : i + 1, :] = traces[k]
    else:
        for i, k in enumerate(near):
            traces[k] = other_traces[i : i + 1, :]
        rows = jnp.concatenate([traces[k] for k in range(len(traces))], axis=0)
        mean = jnp.sum(jnp.sum(weights[...] * rows[None], axis=1), axis=1, keepdims=True)
        out[...] = jnp.broadcast_to(mean, out.shape)


def products(blocks, parts):
    size = parts.shape[1] // 2
    full = jnp.dot(jnp.concatenate(blocks, axis=1), parts, preferred_element_type=F32)
    return (full[size:, size:] + (full[:size, size:] + full[size:, :size])) + full[:size, :size]


def folded(a, b):
    return jnp.sum((a * b).reshape(a.shape[0] // 8, 8, a.shape[1]), axis=0)


def side_by_side(x):
    return jnp.concatenate(split(x), axis=1)


def hold(held, j, value):
    size = value.shape[0]
    start = (j + 1) * size
    at = pl.ds(start if isinstance(j, int) else pl.multiple_of(start, size), size)
    high, remainder = split(value)
    held[at, 0:size] = high
    held[at, size : 2 * size] = remainder


def kept(held, j, count, size):
    start = (j + 1) * size
    return held[pl.ds(start if isinstance(j, int) else pl.multiple_of(start, size), count * size), :]


def coupling(field, low, low_t, out, held):
    per_dev, size = field.shape[0], field.shape[1]
    last = per_dev - 1
    hold(held, 0, field[0])
    hold(held, 1, field[1])
    out[0] = products([low_t[1]], kept(held, 1, 1, size))

    def body(j, carry):
        hold(held, j + 1, field[j + 1])
        parts = jnp.concatenate([kept(held, j - 1, 1, size), kept(held, j + 1, 1, size)], axis=0)
        out[j] = products([low[j], low_t[j + 1]], parts)
        return carry

    lax.fori_loop(1, last, body, 0, unroll=UNROLL)
    out[last] = products([low[last]], kept(held, last - 1, 1, size))


def advance(image, now, mean):
    return (image - mean * now) * (1.0 / mean)


def step_edge(first, field, diag, centre, *rest):
    above, turned, low, low_t = rest[:4]
    top, bottom, to_left = rest[-3:]
    last = field.shape[0] - 1
    if first:
        coupled = rest[4]
        parts = jnp.concatenate([side_by_side(f) for f in (above[0], field[0])], axis=0)
        upper = products([low[0], diag[0]], parts) + coupled[0]
        lower = products([diag[last]], side_by_side(field[last])) + coupled[last] + turned[0]
    else:
        parts = jnp.concatenate([side_by_side(f) for f in (above[0], field[0], field[1])], axis=0)
        upper = products([low[0], diag[0], low_t[1]], parts)
        parts = jnp.concatenate([side_by_side(f) for f in (field[last - 1], field[last])], axis=0)
        lower = products([low[last], diag[last]], parts) + turned[0]
    new = advance(upper, field[0], centre[0:1, :])
    top[0] = new
    to_left[0] = products([low_t[0]], side_by_side(new))
    bottom[0] = advance(lower, field[last], centre[last : last + 1, :])


def step_inner(first, whole, seg, field, diag, centre, *rest):
    if first:
        coupled, edge_top, edge_bottom, out, table, held = rest
    elif whole:
        low, low_t, above, turned, sends = rest[:5]
        tables, out, moments = rest[5 : 4 + ITERS], rest[4 + ITERS], rest[5 + ITERS]
        messages, (table, held) = rest[6 + ITERS : -2], rest[-2:]
    else:
        low, low_t, edge_top, edge_bottom, out, table, held = rest
    per_dev, size = field.shape[0], field.shape[1]
    last = per_dev - 1
    table[...] = jnp.zeros(table.shape, F32)

    def sums(j, now, new):
        system = seg[j]
        table[system, 0] += folded(now, new)
        if not whole:
            table[system, 1] += folded(new, new)
        if first:
            table[system, 2] += folded(now, now)

    def one(j, image):
        now = field[j]
        new = advance(image, now, centre[pl.ds(j, 1), :])
        out[j] = new
        sums(j, now, new)

    def body(j, carry):
        if first:
            one(j, products([diag[j]], side_by_side(field[j])) + coupled[j])
        else:
            hold(held, j + 1, field[j + 1])
            one(j, products([low[j], diag[j], low_t[j + 1]], kept(held, j - 1, 3, size)))
        return carry

    if not first:
        hold(held, 0, field[0])
        hold(held, 1, field[1])
    if whole:
        hold(held, -1, above[0])
        one(0, products([low[0], diag[0], low_t[1]], kept(held, -1, 3, size)))
    else:
        out[0] = edge_top[0]
        sums(0, field[0], edge_top[0])
    lax.fori_loop(1, last, body, 0, unroll=UNROLL)
    if whole:
        one(last, products([low[last], diag[last]], kept(held, last - 1, 2, size)) + turned[0])
        gather_sums(sends, (*tables, table), moments, messages)
    else:
        out[last] = edge_bottom[0]
        sums(last, field[last], edge_bottom[0])


def gather_sums(sends, tables, moments, messages):
    moments[0] = jnp.sum(tables[0][:, 2], axis=1)
    for i, table in enumerate(tables):
        for m in range(2 if i + 1 < len(tables) else 1):
            moments[2 * i + 1 + m] = jnp.sum(table[:, m], axis=1)
    for i, message in enumerate(messages):
        for k in range(2 * len(tables)):
            message[k : k + 1, :] = moments[k, pl.ds(sends[i], 1), :]


def finish(reach, seg, meets, moments, *rest):
    received = rest[: 2 * reach]
    bases = rest[2 * reach : 2 * reach + ITERS + 1]
    centre, sol, res, coef = rest[2 * reach + ITERS + 1 :]
    rows = sol.shape[0]
    systems = moments.shape[1]

    @pl.when(pl.program_id(0) == 0)
    def _():
        index = lax.broadcasted_iota(jnp.int32, (systems, moments.shape[2]), 0)
        m = []
        for k in range(2 * ITERS):
            total = moments[k]
            for i in range(2 * reach):
                total = total + jnp.where(index == meets[i], received[i][k : k + 1, :], 0.0)
            m.append(total)

        def inner(a, b):
            by_degree = {}
            for i, u in enumerate(a):
                for j, v in enumerate(b):
                    by_degree[i + j] = u * v if i + j not in by_degree else by_degree[i + j] + u * v
            return functools.reduce(lambda x, y: x + y, [w * m[d] for d, w in by_degree.items()])

        def ratio(a, b):
            good = (a > 0) & (b > 0)
            return jnp.where(good, a / jnp.where(good, b, 1.0), 0.0)

        one = jnp.ones_like(m[0])
        remains, along, summed = [one], [one], []
        norm = m[0]
        for step in range(ITERS):
            image = [along[0]] + [along[i] + along[i - 1] for i in range(1, len(along))] + [along[-1]]
            size = ratio(norm, inner(along, image))
            summed = [size * a + (summed[i] if i < len(summed) else 0.0) for i, a in enumerate(along)]
            remains = [(remains[i] if i < len(remains) else 0.0) - size * a for i, a in enumerate(image)]
            if step + 1 < ITERS:
                norm_next = inner(remains, remains)
                grow = ratio(norm_next, norm)
                along = [a + (grow * along[i] if i < len(along) else 0.0) for i, a in enumerate(remains)]
                norm = norm_next
        for i in range(ITERS):
            coef[i] = summed[i]
        for i in range(ITERS + 1):
            coef[ITERS + i] = remains[i]

    for j in range(rows):
        row = pl.program_id(0) * rows + j
        system = seg[row]
        values = [basis[j] for basis in bases]
        mean = centre[pl.ds(row, 1), :]
        pick = lambda i: coef[i, pl.ds(system, 1), :]
        inverse = 1.0 / mean
        sol[j] = functools.reduce(
            lambda x, y: x + y, [(pick(i) * inverse) * values[i] for i in reversed(range(ITERS))]
        )
        res[j] = functools.reduce(
            lambda x, y: x + y, [pick(ITERS + i) * values[i] for i in reversed(range(ITERS + 1))]
        )


def body(placing, lengths, diag_blocks, lower_blocks, right_side):
    count = lax.axis_size("row")
    device = lax.axis_index("row")
    per_dev, size = diag_blocks.shape[0], diag_blocks.shape[1]
    width = right_side.shape[2]
    share = per_dev // count
    systems = lengths.shape[0]
    total = count * per_dev
    reach = min(count - 1, -(-(MOSTLEN - 1) // per_dev))
    half = size // 2
    swaps = [1, -1, 2, -2]
    slots = jnp.arange(per_dev, dtype=jnp.int32)
    earlier = slots[None, :] < slots[:, None]

    distances = sorted(range(1, count), key=lambda k: -min(k, count - k))
    far = [k for k in distances if 4 * min(k, count - k) > count]
    near = [0] + [k for k in distances if k not in far]
    coupled_shape = (2 * share, size, width)
    coupled = [None] * count
    *sent, order = call(
        functools.partial(pack_coupled, count, share),
        [sds(coupled_shape)] * count + [sds((per_dev,), jnp.int32)],
        [SMEM, HBM, HBM],
        [HBM] * count + [SMEM],
        [
            pltpu.SMEM((count,), jnp.int32),
            pltpu.VMEM((count,) + coupled_shape, F32),
            pltpu.SemaphoreType.DMA((count,)),
            pltpu.SemaphoreType.DMA((count,)),
        ],
        name="pack_coupled",
    )(placing, in_hbm(lower_blocks), in_hbm(right_side))
    coupled[0] = sent[0]
    for k in distances:
        coupled[k] = shifted(sent[k], k)

    ends = jnp.cumsum(lengths)
    order, ends = lax.optimization_barrier((order, ends))
    diag_rows = share * half + 8 * (-(-(share + 1) // 8))
    sent = call(
        functools.partial(pack_diag, count, share),
        [sds((diag_rows, size))] * count,
        [SMEM, HBM, ANY],
        [VMEM] * count,
        [pltpu.VMEM((per_dev, size, size), F32), pltpu.SemaphoreType.DMA((per_dev,))],
        name="pack_diag",
    )(order, in_hbm(diag_blocks), coupled[GATE])
    halves = [sent[0]] + [None] * (count - 1)
    for k in distances:
        halves[k] = shifted(sent[k], k)


    def system_of(rows):
        return jnp.sum((rows[..., None] >= ends).astype(jnp.int32), axis=-1)

    row0 = device * per_dev
    rows = row0 + slots
    seg = system_of(rows)
    keep = (seg != system_of(rows - 1)) | (rows == 0)
    keep = 1 - keep.astype(jnp.int32)
    first_system, last_system = seg[0], seg[per_dev - 1]
    meets, sends = [], []
    for by in swaps:
        row = row0 - (by - 1) * per_dev - 1 if by > 0 else row0 - by * per_dev
        mine = first_system if by > 0 else last_system
        meets.append(jnp.where((row >= 0) & (row < total) & (system_of(row) == mine), mine, -1))
        sends.append(last_system if by > 0 else first_system)
    meets, sends = jnp.stack(meets), jnp.stack(sends)

    table = placing.reshape(count, per_dev)[::-1]
    table = lax.dynamic_slice_in_dim(jnp.concatenate([table, table]), count - 1 - device, count)
    mine = table // per_dev == device
    rank = jnp.sum((earlier[None] & mine[:, None, :]).astype(jnp.int32), axis=2)
    picks = mine[:, None, :] & (rank[:, None, :] == jnp.arange(share, dtype=jnp.int32)[None, :, None])
    dest = jnp.sum(jnp.where(picks, table[:, None, :] - row0, 0), axis=2).reshape(-1)
    in_length = jnp.sum(jnp.where(seg[:, None] == jnp.arange(systems)[None, :], lengths[None, :], 0), axis=1)
    weights = jnp.where(
        seg[:, None, None] == system_of(table)[None], 1.0 / (size * in_length.astype(F32))[:, None, None], 0.0
    )
    weights = jnp.pad(weights, ((0, 0), (0, 0), (0, size - per_dev)))

    seg, keep, sends, meets, dest, weights = lax.optimization_barrier((seg, keep, sends, meets, dest, weights))

    field_shape, row_shape = sds((per_dev, size, width)), sds((1, size, width))
    block_shape = sds((per_dev, 2 * size, size), BF16)
    rhs, low, low_t, to_left, to_right = call(
        functools.partial(unpack_coupled, count, share),
        [field_shape, block_shape, block_shape, row_shape, row_shape],
        [SMEM, SMEM] + [ANY] * count,
        [VMEM] * 5,
        [pltpu.VMEM((count,) + coupled_shape, F32), pltpu.SemaphoreType.DMA((count,))],
        name="unpack_coupled",
    )(dest, keep, *coupled)
    turned = shifted(to_left, -1)
    above = shifted(to_right, 1)
    held = [pltpu.VMEM(((per_dev + 2) * size, 2 * width), BF16)]
    partly = call(
        coupling, field_shape, [VMEM] * 3, VMEM, held, flops=300000000, name="coupling"
    )(rhs, low, low_t)

    near_diag = call(
        functools.partial(unpack_diag, share, near, None),
        [block_shape, sds((len(near), size))],
        [SMEM] + [ANY] * len(near) + [ANY],
        [VMEM] * 2,
        [pltpu.VMEM((len(near), diag_rows, size), F32), pltpu.SemaphoreType.DMA((len(near),))],
        name="unpack_diag_near",
    )(dest, *[halves[k] for k in near], partly)
    diag, centre = call(
        functools.partial(unpack_diag, share, near, far),
        [block_shape, sds((per_dev, width))],
        [SMEM, VMEM, VMEM, VMEM] + [ANY] * len(far),
        [VMEM] * 2,
        [pltpu.VMEM((len(far), diag_rows, size), F32), pltpu.SemaphoreType.DMA((len(far),))],
        name="unpack_diag_far",
    )(dest, weights, *near_diag, *[halves[k] for k in far])

    bases, tables = [rhs], []
    for i in range(ITERS):
        field = bases[-1]
        first, whole = i == 0, i + 1 == ITERS
        common = (field, diag, centre)
        if not whole:
            extra = (above, turned, low, low_t) + ((partly,) if first else ())
            top, bottom, to_left = call(
                functools.partial(step_edge, first),
                [row_shape] * 3,
                [VMEM] * (3 + len(extra)),
                [VMEM] * 3,
                name="step_edge",
            )(*common, *extra)
        if first:
            extra = (partly, top, bottom)
        elif whole:
            extra = (low, low_t, above, turned)
        else:
            extra = (low, low_t, top, bottom)
        results = [field_shape, sds((systems, 3 if first else 2, 8, width))]
        specs = [SMEM] + [VMEM] * (3 + len(extra))
        room = held
        if whole:
            extra += (sends, *tables)
            specs += [SMEM] + [VMEM] * len(tables)
            room = [pltpu.VMEM(results.pop().shape, F32)] + held
            results += [sds((2 * ITERS, systems, width))] + [sds((2 * ITERS, width))] * len(swaps)
        new, *sums = call(
            functools.partial(step_inner, first, whole),
            results,
            specs,
            [VMEM] * len(results),
            room,
            flops=400000000,
            name="step_inner",
        )(seg, *common, *extra)
        if not whole:
            above = shifted(bottom, 1)
            turned = shifted(to_left, -1)
            tables.append(sums[0])
        bases.append(new)

    moments, *messages = sums
    received = [shifted(message, swap) for message, swap in zip(messages, swaps)]

    step = math.gcd(per_dev, 16)
    block = pl.BlockSpec((step, size, width), lambda i: (i, 0, 0))
    return pl.pallas_call(
        functools.partial(finish, reach),
        out_shape=[field_shape] * 2,
        grid=(per_dev // step,),
        in_specs=[SMEM, SMEM, VMEM] + [VMEM] * (2 * reach) + [block] * (ITERS + 1) + [VMEM],
        out_specs=[block] * 2,
        scratch_shapes=[pltpu.VMEM((2 * ITERS + 1, systems, width), F32)],
        compiler_params=pltpu.CompilerParams(vmem_limit_bytes=20 * MIB),
        name="finish",
    )(seg, meets, moments, *received, *bases, centre)


def solution(mesh):
    spec = P(("grp", "row"), None, None)
    return jax.shard_map(
        lambda *args: tuple(body(*args)),
        mesh=mesh,
        in_specs=(P("grp"), P("grp"), spec, spec, spec),
        out_specs=(spec, spec),
        check_vma=False,
    )
```
